32 devices in a mesh: cuts: 4 (over x, core), exp: 2 (over y), fsdp: 4 (over z).
Axes of the slice: x: 2, y: 2, z: 4, core: 2. Of those that a mesh axis runs over, the one named last changes fastest.
Arguments:
- tokens: bfloat16 [4096, 4096], P(('cuts', 'exp', 'fsdp')), may hold values from -6 to 6
- out_grad: bfloat16 [4096, 4096], P(('cuts', 'exp', 'fsdp')), may hold values from -6 to 6
- expert_ids: int32 [4096, 2], P(('cuts', 'exp', 'fsdp')), may hold values from 0 to 7, as said below
- gate_probs: bfloat16 [4096, 2], P(('cuts', 'exp', 'fsdp')), may hold values from 0.049804688 to 0.94921875
- params: float32 [3, 8, 4096, 256], P(None, 'exp', ('cuts', 'fsdp')), may hold values from -0.1875 to 0.1875
- moment_first: float32 [3, 8, 4096, 256], P(None, 'exp', ('cuts', 'fsdp')), may hold values from -60 to 60
- moment_second: float32 [3, 8, 4096, 256], P(None, 'exp', ('cuts', 'fsdp')), may hold values from 64 to 1024
Outputs:
- token_grad: bfloat16 [4096, 4096], P(('cuts', 'exp', 'fsdp'))
- gate_grad: bfloat16 [4096, 2], P(('cuts', 'exp', 'fsdp'))
- new_params: float32 [3, 8, 4096, 256], P(None, 'exp', ('cuts', 'fsdp'))
- new_first: float32 [3, 8, 4096, 256], P(None, 'exp', ('cuts', 'fsdp'))
- new_second: float32 [3, 8, 4096, 256], P(None, 'exp', ('cuts', 'fsdp'))
The draws below stay inside these ranges and needn't reach their ends.
Inputs may be any that keep to these rules, and one draw needn't show every extreme that they name: `expert_ids`: the two ids of a token differ. Among the tokens of one device no expert is named more than 40 times. Each device names some expert exactly 40 times, and the devices that share their cuts and fsdp indices have one such expert in common.
All inputs are finite; a program needn't handle non-finite values.
Results may differ from the reference program's by a relative error of at most 0.0079.
Values may be sent and summed in bfloat16 or wider, within the bound.
A program may use at most 192 MiB of HBM per device.

```python
import math
import jax
import jax.numpy as jnp
from jax import lax

D = 4096
EXPERTS = 8
F = 256
TOK_DEV = 128
CAP = 40
SENDERS = 2
SHARDS = 4
TOKENS = 4096


def draw_expert_ids(key, part):
    blocks = TOKENS // TOK_DEV
    unit = TOK_DEV // 32
    groups = blocks // SENDERS
    pattern = jnp.array([10, 9, 9, 8, 8, 7, 7, 6], jnp.int32) * unit
    shifts = jax.random.randint(jax.random.fold_in(key, 11), (blocks, 3), -unit, unit + 1).astype(jnp.int32)
    nothing = jnp.zeros((blocks,), jnp.int32)
    delta = jnp.stack([nothing, shifts[:, 0], -shifts[:, 0], shifts[:, 1], -shifts[:, 1], shifts[:, 2], -shifts[:, 2], nothing], axis=1)
    counts = pattern[None, :] + delta
    ends = jnp.cumsum(counts, axis=1)
    position = jnp.arange(2 * TOK_DEV, dtype=jnp.int32)
    pattern_slot = jnp.sum((position[None, :, None] >= ends[:, None, :]).astype(jnp.int32), axis=2)
    block_number = jnp.arange(blocks, dtype=jnp.int32)
    group_number = block_number // (SENDERS * SHARDS) * SHARDS + block_number % SHARDS
    full_expert = jax.random.randint(jax.random.fold_in(key, 12), (groups,), 0, 8).astype(jnp.int32)[group_number]
    order_keys = jax.random.split(jax.random.fold_in(key, 13), blocks)
    orders = jax.vmap(lambda one: jax.random.permutation(one, 8))(order_keys).astype(jnp.int32)
    labels = (orders - orders[:, :1] + full_expert[:, None]) % 8
    named = jnp.take_along_axis(labels, pattern_slot, axis=1)
    first_half = named[:, :TOK_DEV]
    second_half = named[:, TOK_DEV:]
    flipped = jax.random.randint(jax.random.fold_in(key, 14), (blocks, TOK_DEV), 0, 2).astype(jnp.int32)
    paired = jnp.stack([jnp.where(flipped == 1, second_half, first_half), jnp.where(flipped == 1, first_half, second_half)], axis=-1)
    shuffle_keys = jax.random.split(jax.random.fold_in(key, 15), blocks)
    shuffles = jax.vmap(lambda one: jax.random.permutation(one, TOK_DEV))(shuffle_keys).astype(jnp.int32)
    paired = jnp.take_along_axis(paired, shuffles[:, :, None], axis=1)
    return paired.reshape(TOKENS, 2).astype(jnp.int32)


def with_spikes(values, stream_key, source, target, parts, factor):
    def block_of(dim):
        return (jnp.arange(values.shape[dim]) // (values.shape[dim] // parts)).reshape((-1,) + (1,) * (values.ndim - 1 - dim))

    near = jax.random.permutation(stream_key, parts)[block_of(target)]
    other_side = (block_of(target) + parts // 2) % parts
    return jnp.where((block_of(source) == near) | (block_of(source) == other_side), factor * values, values)


def steps_of(key, extent, shards, low, top_value):
    factor_of, own = 1.0, jax.random.fold_in(key, 6)
    for dim, shards_of in shards:
        draws = jnp.exp(jax.random.uniform(jax.random.fold_in(own, dim), (shards_of,), jnp.float32, low / len(shards), top_value / len(shards)))
        factor_of = factor_of * jnp.repeat(draws, extent[dim] // shards_of).reshape([-1 if axis == dim else 1 for axis in range(len(extent))])
    return factor_of


def noise(rng, shape, scale, most, cuts=(), kind=jnp.bfloat16):
    result = jax.random.normal(rng, shape, jnp.float32) * scale
    if len(cuts) > 0:
        result = steps_of(rng, shape, cuts, -0.22, 0.18) * result
    return jnp.clip(result, min=-most, max=most).astype(kind)


def heavy_noise(key, extent, scale, most, cuts, heavy, kind=jnp.bfloat16):
    result = scale * jax.random.normal(key, extent, jnp.float32)
    if cuts:
        result = result * steps_of(key, extent, cuts, -0.22, 0.18)
    return jnp.clip(with_spikes(result, jax.random.fold_in(key, 3), *heavy), -most, most).astype(kind)


def setup_inputs(seed: int = 0) -> dict:
    splits = jax.random.split(jax.random.key(seed), 8)
    tokens = noise(splits[0], (TOKENS, D), 1.0, 6.0, ((0, 32),))
    out_grad = heavy_noise(splits[1], (TOKENS, D), 1.0, 6.0, ((0, 32),), (0, 1, 32, 2.75))
    expert_ids = draw_expert_ids(jax.random.fold_in(splits[7], 71), 0)
    gate_probs = jnp.clip(0.049804688 + 0.89941406 * jax.random.uniform(splits[3], (TOKENS, 2), jnp.float32) ** steps_of(splits[3], (TOKENS, 2), ((0, 32),), -0.2, 0.2), 0.049804688, 0.94921875).astype(jnp.bfloat16)
    params = noise(splits[4], (3, EXPERTS, D, F), (D // 4) ** -0.5, 0.1875, ((1, 2), (2, 16)), jnp.float32)
    moment_first = noise(splits[5], (3, EXPERTS, D, F), 10.0, 60.0, ((1, 2), (2, 16)), jnp.float32)
    moment_second = jnp.clip(jnp.exp(math.log(1024.0) - 2.7725887 * jax.random.uniform(splits[6], (3, EXPERTS, D, F), jnp.float32) ** steps_of(splits[6], (3, EXPERTS, D, F), ((1, 2), (2, 16)), -0.2, 0.2)), 64.0, 1024.0)
    return dict(tokens=tokens, out_grad=out_grad, expert_ids=expert_ids, gate_probs=gate_probs, params=params, moment_first=moment_first, moment_second=moment_second)


decay_first = 0.9
decay_second = 0.95
correct_first = 1.0 - 0.9 ** 10
correct_second = 1.0 - 0.95 ** 10
epsilon = 1e-08
learn_rate = 0.0003
weight_decay = 0.1

def adam_update(params, gradient, moment_first, moment_second):
    new_first = decay_first * moment_first + (1.0 - decay_first) * gradient
    new_second = decay_second * moment_second + (1.0 - decay_second) * gradient * gradient
    stepped = new_first / correct_first / (jnp.sqrt(new_second / correct_second) + epsilon)
    new_params = params - learn_rate * (stepped + weight_decay * params)
    return (new_params, new_first, new_second)

def reference(tokens, out_grad, expert_ids, gate_probs, params, moment_first, moment_second):
    weights = params.astype(jnp.bfloat16)
    token_count = tokens.shape[0]
    slots_most = CAP * (TOKENS // TOK_DEV)
    flat_ids = expert_ids.reshape(-1)
    flat_gate = gate_probs.reshape(-1)

    def expert_step(totals, expert):
        token_acc, gate_acc = totals
        chosen = flat_ids == expert
        picked = jnp.nonzero(chosen, size=slots_most, fill_value=0)[0].astype(jnp.int32)
        filled = jnp.arange(slots_most, dtype=jnp.int32) < jnp.sum(chosen.astype(jnp.int32))
        token_rows = picked // 2
        inputs = tokens[token_rows]
        upstream = out_grad[token_rows]
        gate_values = jnp.where(filled, flat_gate[picked], jnp.zeros((), flat_gate.dtype)).astype(jnp.float32)[:, None]
        w_gate = weights[0, expert]
        w_up = weights[1, expert]
        w_down = weights[2, expert]
        pre_gate = jnp.dot(inputs, w_gate, preferred_element_type=jnp.float32)
        pre_up = jnp.dot(inputs, w_up, preferred_element_type=jnp.float32)
        sigmoid_gate = jax.nn.sigmoid(pre_gate)
        activated = pre_gate * sigmoid_gate
        hidden = activated * pre_up
        projected = jnp.dot(upstream, w_down, preferred_element_type=jnp.float32)
        slot_gate = lax.optimization_barrier(jnp.sum(hidden * projected, axis=1)).astype(jnp.bfloat16)
        delta_hidden = gate_values * projected
        delta_gate = (delta_hidden * pre_up * sigmoid_gate * (1.0 + pre_gate * (1.0 - sigmoid_gate))).astype(jnp.bfloat16)
        delta_up = (delta_hidden * activated).astype(jnp.bfloat16)
        scaled = (gate_values * upstream.astype(jnp.float32)).astype(jnp.bfloat16)
        slot_grads = (jnp.dot(delta_gate, w_gate.T, preferred_element_type=jnp.float32) + jnp.dot(delta_up, w_up.T, preferred_element_type=jnp.float32)).astype(jnp.bfloat16)
        grad_gate = jnp.dot(inputs.T, delta_gate, preferred_element_type=jnp.float32)
        grad_up = jnp.dot(inputs.T, delta_up, preferred_element_type=jnp.float32)
        grad_down = jnp.dot(scaled.T, hidden.astype(jnp.bfloat16), preferred_element_type=jnp.float32)
        token_acc = token_acc.at[token_rows].add(jnp.where(filled[:, None], slot_grads.astype(jnp.float32), jnp.zeros((), jnp.float32)))
        gate_acc = gate_acc.at[picked].add(jnp.where(filled, slot_gate.astype(jnp.float32), jnp.zeros((), jnp.float32)))
        return ((token_acc, gate_acc), jnp.stack([grad_gate, grad_up, grad_down]))
    start = (jnp.zeros(tokens.shape, jnp.float32), jnp.zeros((token_count * 2,), jnp.float32))
    (token_acc, gate_acc), gradient = lax.scan(expert_step, start, jnp.arange(EXPERTS, dtype=jnp.int32))
    gradient = jnp.transpose(gradient, (1, 0, 2, 3))
    new_params, new_first, new_second = adam_update(params, gradient, moment_first, moment_second)
    return (token_acc.astype(jnp.bfloat16), gate_acc.reshape(token_count, 2).astype(jnp.bfloat16), new_params, new_first, new_second)
```

```python
import jax
import jax.numpy as jnp
from jax import lax
from jax.sharding import PartitionSpec as P

EXPERTS = 8


decay_first = 0.9
decay_second = 0.95
correct_first = 1.0 - 0.9**10
correct_second = 1.0 - 0.95**10
epsilon = 1e-08
learn_rate = 0.0003
weight_decay = 0.1
GROUP = ("cuts", "fsdp")


def adam_update(params, gradient, moment_first, moment_second):
    new_first = decay_first * moment_first + (1.0 - decay_first) * gradient
    new_second = decay_second * moment_second + (1.0 - decay_second) * gradient * gradient
    stepped = new_first / correct_first / (jnp.sqrt(new_second / correct_second) + epsilon)
    new_params = params - learn_rate * (stepped + weight_decay * params)
    return (new_params, new_first, new_second)


def per_device(tokens, out_grad, expert_ids, gate_probs, params, moment_first, moment_second):
    token_count, width = tokens.shape
    local = params.shape[1]
    rows = params.shape[2]
    hidden_units = params.shape[3]
    shares = width // rows
    exp_count = lax.axis_size("exp")
    capacity = 10 * token_count // 32
    me = lax.axis_index("exp")
    local_slots = local * capacity

    weights = params.astype(jnp.bfloat16)
    w_in = jnp.concatenate([weights[0], weights[1]], axis=2)
    w_down = weights[2]

    cores = 2
    cuts = lax.axis_size("cuts")
    shards = lax.axis_size("fsdp")
    chips = cuts // cores
    core_groups = [[chip * cores + core for core in range(cores)] for chip in range(chips)]
    chip_groups = [
        [(chip * cores + core) * shards + shard for chip in range(chips) for shard in range(shards)]
        for core in range(cores)
    ]

    def spread(array):
        parts = array.reshape(array.shape[0], shares, rows).transpose(1, 0, 2)
        return parts

    def exchange(parts):
        parts = lax.all_to_all(parts, GROUP, split_axis=0, concat_axis=0, tiled=True)
        return lax.all_gather(parts, "exp", axis=1, tiled=False)

    flat_ids = expert_ids.reshape(-1)
    onehot = (flat_ids[:, None] == jnp.arange(EXPERTS, dtype=jnp.int32)).astype(jnp.int32)
    before = jnp.cumsum(onehot, axis=0) - onehot
    position = jnp.sum(before * onehot, axis=1)
    extra = jnp.concatenate(
        [flat_ids.astype(jnp.bfloat16), position.astype(jnp.bfloat16), gate_probs.reshape(-1)]
    )
    extra_rows = extra.shape[0] // rows
    padded = -(-extra_rows // 8) * 8
    extra = jnp.pad(extra.reshape(extra_rows, rows), ((0, padded - extra_rows), (0, 0)))
    extra = jnp.broadcast_to(extra[None], (shares, padded, rows))

    sources = shares * exp_count
    token_parts = exchange(jnp.concatenate([spread(tokens), extra], axis=1))
    upstream_parts = exchange(spread(out_grad))
    everyone = token_parts[:, :, token_count : token_count + extra_rows, :]
    everyone = everyone.reshape(sources, 3, token_count, 2)
    ids = everyone[:, 0].astype(jnp.int32)
    all_slots = ids * capacity + everyone[:, 1].astype(jnp.int32) - me * local_slots
    all_gates = everyone[:, 2].astype(jnp.float32)
    columns = jnp.arange(local_slots, dtype=jnp.int32)
    place = (all_slots[:, :, :, None] == columns).astype(jnp.bfloat16).sum(axis=2)

    def pick(array):
        array = array[:, :, :token_count].reshape(sources, token_count, rows)
        picked = jnp.einsum("ntc,ntd->ncd", place, array, preferred_element_type=jnp.bfloat16)
        picked = picked.reshape(sources, local, capacity, rows).transpose(1, 0, 2, 3)
        return picked.reshape(local, sources * capacity, rows)

    inputs = pick(token_parts)
    upstream = pick(upstream_parts)

    def partial_sums(left, right):
        out = jnp.einsum("esd,edf->esf", left, right, preferred_element_type=jnp.float32)
        out = out.astype(jnp.bfloat16)
        out = out.reshape(local, chips, cores, shards, exp_count * capacity, right.shape[2])
        out = out.transpose(2, 1, 3, 0, 4, 5)
        out = lax.all_to_all(
            out, "cuts", split_axis=0, concat_axis=0, tiled=True, axis_index_groups=core_groups
        )
        out = jnp.sum(out.astype(jnp.float32), axis=0).astype(jnp.bfloat16)
        out = out.reshape((chips * shards,) + out.shape[2:])
        out = lax.all_to_all(
            out, GROUP, split_axis=0, concat_axis=0, tiled=True, axis_index_groups=chip_groups
        )
        return jnp.sum(out.astype(jnp.float32), axis=0)

    pre = partial_sums(inputs, w_in)
    projected = partial_sums(upstream, w_down)
    pre_gate = pre[:, :, :hidden_units]
    pre_up = pre[:, :, hidden_units:]

    start = lax.axis_index(GROUP) * exp_count
    my_slots = lax.dynamic_slice_in_dim(all_slots, start, exp_count, axis=0)
    my_gates = lax.dynamic_slice_in_dim(all_gates, start, exp_count, axis=0)
    my_place = (my_slots[:, :, :, None] == columns).astype(jnp.float32)
    gates = jnp.sum(my_place * my_gates[:, :, :, None], axis=(1, 2))
    gates = gates.reshape(exp_count, local, capacity).transpose(1, 0, 2)
    gates = gates.reshape(local, exp_count * capacity, 1)

    sigmoid_gate = jax.nn.sigmoid(pre_gate)
    activated = pre_gate * sigmoid_gate
    hidden = activated * pre_up
    slot_gate = jnp.sum(hidden * projected, axis=2)
    delta_hidden = gates * projected
    delta_gate = delta_hidden * pre_up * sigmoid_gate * (1.0 + pre_gate * (1.0 - sigmoid_gate))
    delta_up = delta_hidden * activated
    deltas = jnp.concatenate([delta_gate, delta_up, gates * hidden], axis=2).astype(jnp.bfloat16)
    deltas = lax.all_gather(deltas, GROUP, axis=0, tiled=False)
    deltas = deltas.transpose(1, 0, 2, 3).reshape(local, sources * capacity, 3 * hidden_units)
    delta_in = deltas[:, :, : 2 * hidden_units]
    scaled_hidden = deltas[:, :, 2 * hidden_units :]

    slot_gate = slot_gate.reshape(local, exp_count, capacity).transpose(1, 0, 2)
    slot_gate = slot_gate.reshape(exp_count, 1, 1, local_slots)
    gate_part = jnp.sum(my_place * slot_gate, axis=3)
    gate_part = gate_part.astype(jnp.bfloat16).reshape(exp_count, token_count * 2)
    gate_part = lax.all_to_all(gate_part, "exp", split_axis=0, concat_axis=0, tiled=True)
    gate_grad = jnp.sum(gate_part.astype(jnp.float32), axis=0).astype(jnp.bfloat16)
    gate_grad = gate_grad.reshape(token_count, 2)

    slot_grads = jnp.einsum("esf,edf->esd", delta_in, w_in, preferred_element_type=jnp.float32)
    slot_grads = slot_grads.astype(jnp.bfloat16).reshape(local, sources, capacity, rows)
    slot_grads = slot_grads.transpose(1, 0, 2, 3).reshape(sources, local_slots, rows)
    returned = jnp.einsum("ntc,ncd->ntd", place, slot_grads, preferred_element_type=jnp.bfloat16)
    returned = returned.reshape(shares, exp_count, token_count, rows)
    returned = lax.all_to_all(returned, "exp", split_axis=1, concat_axis=1, tiled=True)
    returned = jnp.sum(returned.astype(jnp.float32), axis=1).astype(jnp.bfloat16)
    returned = lax.all_to_all(returned, GROUP, split_axis=0, concat_axis=0, tiled=True)
    token_grad = returned.transpose(1, 0, 2).reshape(token_count, width)

    grad_in = jnp.einsum("esd,esf->edf", inputs, delta_in, preferred_element_type=jnp.float32)
    grad_down = jnp.einsum(
        "esd,esf->edf", upstream, scaled_hidden, preferred_element_type=jnp.float32
    )
    gradient = jnp.stack([grad_in[:, :, :hidden_units], grad_in[:, :, hidden_units:], grad_down])
    new_params, new_first, new_second = adam_update(params, gradient, moment_first, moment_second)
    return (token_grad, gate_grad, new_params, new_first, new_second)


def solution(mesh):
    tokens_spec = P(("cuts", "exp", "fsdp"), None)
    weights_spec = P(None, "exp", ("cuts", "fsdp"), None)
    return jax.shard_map(
        per_device,
        mesh=mesh,
        in_specs=(tokens_spec,) * 4 + (weights_spec,) * 3,
        out_specs=(tokens_spec,) * 2 + (weights_spec,) * 3,
        check_vma=False,
    )
```
